32 devices in a mesh: row: 8 (over z, x), col: 2 (over y), depth: 2 (over core).
Axes of the slice: x: 2, y: 2, z: 4, core: 2. Of those that a mesh axis runs over, the one named last changes fastest.
Arguments:
- tokens: bfloat16 [1024, 5376], P('row', 'depth'), may hold values from -6 to 6
- gate_weight: bfloat16 [9216, 5376], P(('col', 'row'), 'depth'), may hold values from -0.078125 to 0.078125
- up_weight: bfloat16 [9216, 5376], P(('col', 'row'), 'depth'), may hold values from -0.078125 to 0.078125
- down_weight: bfloat16 [9216, 5376], P(('col', 'depth'), 'row'), may hold values from -0.09375 to 0.09375
Outputs:
- output: bfloat16 [1024, 5376], P('row', ('col', 'depth'))
The draws below stay inside these ranges and needn't reach their ends.
All inputs are finite; a program needn't handle non-finite values.
Results may differ from the reference program's by a relative error of at most 0.0049.
Values may be sent and summed in bfloat16 or wider, within the bound.
A program may use at most 128 MiB of HBM per device.

```python
import jax
import jax.numpy as jnp

D = 5376
FFW = 9216
TOKENS = 1024


def strengthened(result, key, source, target, parts, factor):
    def block_of(dim):
        return (jnp.arange(result.shape[dim]) // (result.shape[dim] // parts)).reshape((-1,) + (1,) * (result.ndim - 1 - dim))

    one_side = jax.random.permutation(key, parts)[block_of(target)]
    second = (block_of(target) + parts // 2) % parts
    return jnp.where((block_of(source) == one_side) | (block_of(source) == second), factor * result, result)


def level_of(own_key, extent, split, smallest, largest):
    factor_of, own = 1.0, jax.random.fold_in(own_key, 6)
    for axis_at, blocks in split:
        draws = jnp.exp(jax.random.uniform(jax.random.fold_in(own, axis_at), (blocks,), jnp.float32, smallest / len(split), largest / len(split)))
        factor_of = factor_of * jnp.repeat(draws, extent[axis_at] // blocks).reshape([-1 if axis == axis_at else 1 for axis in range(len(extent))])
    return factor_of


def gaussian(rng, dims, spread, limit, pieces=(), held_as=jnp.bfloat16):
    loudness = level_of(rng, dims, pieces, -0.22, 0.18) if pieces else 1.0
    result = jax.random.normal(rng, dims, jnp.float32) * spread * loudness
    return jnp.minimum(jnp.maximum(result, -limit), limit).astype(held_as)


def noise_with(key, dims, spread, most, shards, heavy, dtype=jnp.bfloat16):
    result = spread * jax.random.normal(key, dims, jnp.float32)
    if shards:
        result = result * level_of(key, dims, shards, -0.22, 0.18)
    return jnp.clip(strengthened(result, jax.random.fold_in(key, 3), *heavy), -most, most).astype(dtype)


def setup_inputs(seed: int = 0) -> dict:
    key_of = jax.random.split(jax.random.key(seed), 5)
    tokens = gaussian(key_of[0], (TOKENS, D), 1.0, 6.0, ((0, 8), (1, 2)))
    gate_weight = gaussian(key_of[1], (FFW, D), D ** -0.5, 0.078125, ((0, 16), (1, 2)))
    up_weight = gaussian(key_of[2], (FFW, D), D ** -0.5, 0.078125, ((0, 16), (1, 2)))
    down_weight = noise_with(key_of[3], (FFW, D), FFW ** -0.5, 0.09375, ((0, 4), (1, 8)), (0, 1, 8, 2.0))
    return dict(tokens=tokens, gate_weight=gate_weight, up_weight=up_weight, down_weight=down_weight)


def reference(tokens, gate_weight, up_weight, down_weight):
    gate_part = jnp.dot(tokens, gate_weight.T, preferred_element_type=jnp.float32)
    up_part = jnp.dot(tokens, up_weight.T, preferred_element_type=jnp.float32)
    hidden = (jax.nn.silu(gate_part) * up_part).astype(jnp.bfloat16)
    return jnp.dot(hidden, down_weight, preferred_element_type=jnp.float32).astype(jnp.bfloat16)
```

```python
import jax
import jax.numpy as jnp
from jax import lax
from jax.sharding import PartitionSpec as P


def send_out(partial, rows, cols, depths):
    quarters = cols * depths
    per = rows // quarters
    mine = lax.psum_scatter(partial, ("col", "depth"), scatter_dimension=0, tiled=True)
    mine = mine.astype(jnp.bfloat16)
    block = mine.shape[0] // per
    width = mine.shape[1]
    row = lax.axis_index("row")
    low = row % per
    got = jnp.zeros((block, per, width), jnp.bfloat16)
    for k in range(per):
        pairs = []
        for r in range(rows):
            for q in range(quarters):
                a, e = r // per, r % per
                to_row = q * per + (e + k) % per
                pairs.append((r * quarters + q, to_row * quarters + a))
        piece = lax.dynamic_slice_in_dim(mine, (low + k) % per * block, block, 0)
        piece = lax.ppermute(piece, ("row", "col", "depth"), pairs)
        got = lax.dynamic_update_slice_in_dim(got, piece[:, None], (low - k) % per, 1)
    return got.reshape(block, per * width)


def solution(mesh):
    rows, cols, depths = (mesh.shape[a] for a in ("row", "col", "depth"))

    def local(tokens, gate_weight, up_weight, down_weight):
        units = gate_weight.shape[0]
        every = lax.all_gather(tokens, "row", axis=0, tiled=True)
        down = down_weight.reshape(rows // depths, depths, units // depths, -1)
        down = lax.all_to_all(down, "depth", split_axis=1, concat_axis=0, tiled=True)
        down = down.reshape(rows, units // depths, -1)
        paired = jnp.stack([gate_weight, up_weight])
        sums = jnp.einsum("td,gfd->gtf", every, paired, preferred_element_type=jnp.float32)
        sums = lax.psum_scatter(sums, "depth", scatter_dimension=2, tiled=True)
        hidden = (jax.nn.silu(sums[0]) * sums[1]).astype(jnp.bfloat16)
        hidden = lax.all_gather(hidden, "row", axis=0)
        partial = jnp.einsum("rtk,rkc->tc", hidden, down, preferred_element_type=jnp.float32)
        return send_out(partial, rows, cols, depths)

    in_specs = (
        P("row", "depth"),
        P(("col", "row"), "depth"),
        P(("col", "row"), "depth"),
        P(("col", "depth"), "row"),
    )
    out_specs = P("row", ("col", "depth"))
    return jax.shard_map(local, mesh=mesh, in_specs=in_specs, out_specs=out_specs, check_vma=False)
```

```python
import functools

import jax
import jax.numpy as jnp
from jax import lax
from jax.experimental import pallas as pl
from jax.experimental.pallas import tpu as pltpu
from jax.sharding import PartitionSpec as P

MESH = pl.DeviceIdType.MESH
F32 = jnp.float32
BF16 = jnp.bfloat16


def row_at(place, n):
    back = place // (n // 2)
    return 2 * place * (1 - back) + (2 * (n - 1 - place) + 1) * back


def kernel(n, tok_hbm, gate_hbm, up_hbm, down_hbm, out_ref, tok, weights, down, part, theirs, hid,
           total, other, send_y, from_y, load_sem, down_load, down_send, down_recv, tok_send, tok_recv,
           y_send, y_recv, part_send, part_recv, hid_send, hid_recv, sum_send, sum_recv, col_send, col_recv):
    row, col, core = lax.axis_index("row"), lax.axis_index("col"), lax.axis_index("depth")
    half = n // 2
    x, z = row % 2, row // 2
    place = z * (1 - x) + (n - 1 - z) * x
    ways = ({"row": row_at((place + 1) % n, n)}, {"row": row_at((place + n - 1) % n, n)})
    beside, partner = {"col": 1 - col}, {"depth": 1 - core}
    block = tok_hbm.shape[0]
    third = tok_hbm.shape[1] // 3
    units = gate_hbm.shape[0]
    share = units // 2

    def remote(src, dst, send, recv, to):
        return pltpu.make_async_remote_copy(src_ref=src, dst_ref=dst, send_sem=send, recv_sem=recv,
                                            device_id=to, device_id_type=MESH)

    loads = [pltpu.make_async_copy(tok_hbm.at[:, pl.ds(t * third, third)], tok.at[t, 0], load_sem.at[t])
             for t in range(3)]
    loads += [pltpu.make_async_copy(gate_hbm, weights.at[0], load_sem.at[3]),
              pltpu.make_async_copy(up_hbm, weights.at[1], load_sem.at[4])]
    for copy in loads:
        copy.start()
    barrier = pltpu.get_barrier_semaphore()
    for peer in ways + (beside, partner):
        pl.semaphore_signal(barrier, inc=1, device_id=peer, device_id_type=MESH)
    pl.semaphore_wait(barrier, 4)
    for copy in loads[:3]:
        copy.wait()

    def slot(hop, way):
        return 0 if hop == 0 else 1 if hop == half else 2 * hop + way

    def rounds(hop, chunk):
        return (chunk,) if hop == half else (0, 1)

    started = []

    def go(copy):
        copy.start()
        started.append(copy)

    def tok_copy(hop, way, chunk):
        t = 2 * col if chunk == 0 else 1
        return remote(tok.at[t, slot(hop - 1, way)], tok.at[t, slot(hop, way)],
                      tok_send.at[way, hop - 1, chunk], tok_recv.at[way, hop - 1, chunk], ways[way])

    def y_copy(at, t):
        return remote(tok.at[t, at], tok.at[t, at], y_send.at[at], y_recv.at[at], beside)

    for chunk in (0, 1):
        for way in (0, 1):
            go(tok_copy(1, way, chunk))

    local_down, remote_down = [], []
    for i in range(half):
        keep = down_hbm.at[pl.ds(i * units + core * share, share)]
        give = down_hbm.at[pl.ds(i * units + (1 - core) * share, share)]
        dst = down.at[core * half + i]
        local_down.append(pltpu.make_async_copy(keep, dst, down_load.at[i]))
        remote_down.append(remote(give, dst, down_send.at[i], down_recv.at[i], partner))
    for copy in loads[3:]:
        copy.wait()
    for copy in local_down + remote_down:
        copy.start()

    def gate_up(group, slots, places):
        wide = block * len(slots)
        first = slots[0]

        @pl.loop(0, 4)
        def _(step):
            side, kind = step // 2, step % 2
            which = (1 - core) * (1 - side) + core * side
            rows = pl.ds(pl.multiple_of(which * share, 16), share)
            acc = None
            for t in range(3):
                seen = tok[t, first:first + len(slots)].reshape(wide, third)
                term = lax.dot_general(weights[kind, rows, t * third:(t + 1) * third], seen,
                                       (((1,), (1,)), ((), ())), preferred_element_type=F32)
                acc = term if acc is None else acc + term
            part[group, side, kind, :, :wide] = acc

        swap = remote(part.at[group, 0, :, :, pl.ds(0, wide)], theirs.at[group, :, :, pl.ds(0, wide)],
                      part_send.at[group], part_recv.at[group], partner)
        go(swap)
        swap.wait_recv()
        for k, at in enumerate(places):
            lanes = slice(k * block, (k + 1) * block)
            gate = part[group, 1, 0, :, lanes] + theirs[group, 0, :, lanes]
            up = part[group, 1, 1, :, lanes] + theirs[group, 1, :, lanes]
            to = pl.ds(pl.multiple_of(row_at(at, n) * block, block), block)
            hid[0, :, to] = (gate / (1.0 + jnp.exp(-gate)) * up).astype(BF16)

    def pair(hop):
        return [2 * hop, 2 * hop + 1], [(place + n - hop) % n, (place + hop) % n]

    for hop in range(1, half + 1):
        for chunk in (0, 1):
            for way in rounds(hop, chunk):
                tok_copy(hop, way, chunk).wait_recv()
                if hop < half and way in rounds(hop + 1, chunk):
                    go(tok_copy(hop + 1, way, chunk))
                if chunk == 0:
                    go(y_copy(slot(hop, way), 2 * col))
        if hop == 1:
            gate_up(0, [0], [place])
        else:
            slots, places = pair(hop - 1)
            for at in slots:
                y_copy(at, 2 - 2 * col).wait_recv()
            gate_up(hop - 1, slots, places)
    y_copy(1, 2 - 2 * col).wait_recv()
    gate_up(half, [1], [(place + half) % n])

    pieces = 2
    lanes = block * n // pieces

    def hid_copy(hop, way, chunk):
        at = pl.ds(chunk * lanes, lanes)
        return remote(hid.at[slot(hop - 1, way), :, at], hid.at[slot(hop, way), :, at],
                      hid_send.at[way, hop - 1, chunk], hid_recv.at[way, hop - 1, chunk], ways[way])

    for chunk in range(pieces):
        for way in (0, 1):
            go(hid_copy(1, way, chunk))
    for copy in local_down:
        copy.wait()
    for copy in remote_down:
        copy.wait()

    quarter = total.shape[1]

    def add_down(at, source, start):
        of = row_at(source, n)

        @pl.loop(0, total.shape[0])
        def _(q):
            some = hid[at, :, pl.ds(pl.multiple_of(q * quarter, quarter), quarter)]
            term = lax.dot_general(some, down[of], (((0,), (0,)), ((), ())), preferred_element_type=F32)
            total[q] = term if start else total[q] + term

    add_down(0, place, True)
    for hop in range(1, half + 1):
        for chunk in range(pieces):
            for way in rounds(hop, chunk):
                hid_copy(hop, way, chunk).wait_recv()
                if hop < half and way in rounds(hop + 1, chunk):
                    go(hid_copy(hop + 1, way, chunk))
        if hop < half:
            slots, places = pair(hop)
            for at, source in zip(slots, places):
                add_down(at, source, False)
    add_down(1, (place + half) % n, False)

    def sum_copy(c, k):
        return remote(total.at[c * 2 + 1 - core], other.at[c], sum_send.at[k], sum_recv.at[k], partner)

    go(sum_copy(1 - col, 0))
    go(sum_copy(col, 1))
    sum_copy(1 - col, 0).wait_recv()
    send_y[...] = (total[(1 - col) * 2 + core] + other[1 - col]).astype(BF16)
    swap = remote(send_y, from_y, col_send, col_recv, beside)
    go(swap)
    sum_copy(col, 1).wait_recv()
    mine = total[col * 2 + core] + other[col]
    swap.wait_recv()
    out_ref[...] = (mine + from_y[...].astype(F32)).astype(BF16)
    for copy in started:
        copy.wait_send()


def partial_sums(n, tokens, gate_weight, up_weight, down_weight):
    block, width = tokens.shape
    units = gate_weight.shape[0]
    features = down_weight.shape[1]
    half, share = n // 2, units // 2
    every = n * block
    dma = pltpu.SemaphoreType.DMA
    return pl.pallas_call(
        functools.partial(kernel, n),
        out_shape=jax.ShapeDtypeStruct((every // 4, features), BF16),
        in_specs=[pl.BlockSpec(memory_space=pl.ANY)] * 4,
        out_specs=pl.BlockSpec(memory_space=pltpu.VMEM),
        scratch_shapes=[
            pltpu.VMEM((3, n, block, width // 3), BF16),
            pltpu.VMEM((2, units, width), BF16),
            pltpu.VMEM((n, share, features), BF16),
            pltpu.VMEM((half + 1, 2, 2, share, 2 * block), F32),
            pltpu.VMEM((half + 1, 2, share, 2 * block), F32),
            pltpu.VMEM((n, share, every), BF16),
            pltpu.VMEM((4, every // 4, features), F32),
            pltpu.VMEM((2, every // 4, features), F32),
            pltpu.VMEM((every // 4, features), BF16),
            pltpu.VMEM((every // 4, features), BF16),
            dma((5,)),
            dma((half,)), dma((half,)), dma((half,)),
            dma((2, half, 2)), dma((2, half, 2)),
            dma((n,)), dma((n,)),
            dma((half + 1,)), dma((half + 1,)),
            dma((2, half, 2)), dma((2, half, 2)),
            dma((2,)), dma((2,)),
            dma, dma,
        ],
        compiler_params=pltpu.CompilerParams(
            collective_id=0, has_side_effects=True, vmem_limit_bytes=60 * 1024 * 1024
        ),
    )(tokens, gate_weight, up_weight, down_weight)


def send_out(mine, rows, cols, depths):
    quarters = cols * depths
    per = rows // quarters
    block = mine.shape[0] // per
    width = mine.shape[1]
    row = lax.axis_index("row")
    low = row % per
    got = jnp.zeros((block, per, width), jnp.bfloat16)
    for k in range(per):
        pairs = []
        for r in range(rows):
            for q in range(quarters):
                a, e = r // per, r % per
                to_row = q * per + (e + k) % per
                pairs.append((r * quarters + q, to_row * quarters + a))
        piece = lax.dynamic_slice_in_dim(mine, (low + k) % per * block, block, 0)
        piece = lax.ppermute(piece, ("row", "col", "depth"), pairs)
        got = lax.dynamic_update_slice_in_dim(got, piece[:, None], (low - k) % per, 1)
    return got.reshape(block, per * width)


def solution(mesh):
    rows, cols, depths = (mesh.shape[a] for a in ("row", "col", "depth"))

    def local(tokens, gate_weight, up_weight, down_weight):
        units = gate_weight.shape[0]
        every = lax.all_gather(tokens, "row", axis=0, tiled=True)
        down = down_weight.reshape(rows // depths, depths, units // depths, -1)
        down = lax.all_to_all(down, "depth", split_axis=1, concat_axis=0, tiled=True)
        down = down.reshape(rows, units // depths, -1)
        paired = jnp.stack([gate_weight, up_weight])
        sums = jnp.einsum("td,gfd->gtf", every, paired, preferred_element_type=jnp.float32)
        sums = lax.psum_scatter(sums, "depth", scatter_dimension=2, tiled=True)
        hidden = (jax.nn.silu(sums[0]) * sums[1]).astype(jnp.bfloat16)
        hidden = lax.all_gather(hidden, "row", axis=0)
        partial = jnp.einsum("rtk,rkc->tc", hidden, down, preferred_element_type=jnp.float32)
        mine = lax.psum_scatter(partial, ("col", "depth"), scatter_dimension=0, tiled=True)
        return send_out(mine.astype(BF16), rows, cols, depths)

    def fused(*args):
        return send_out(partial_sums(rows, *args), rows, cols, depths)

    in_specs = (
        P("row", "depth"),
        P(("col", "row"), "depth"),
        P(("col", "row"), "depth"),
        P(("col", "depth"), "row"),
    )
    out_specs = P("row", ("col", "depth"))
    small = cols == 2 and depths == 2 and rows % 4 == 0
    return jax.shard_map(fused if small else local, mesh=mesh, in_specs=in_specs, out_specs=out_specs, check_vma=False)
```

```python
import functools

import jax
import jax.numpy as jnp
from jax import lax
from jax.experimental import pallas as pl
from jax.experimental.pallas import tpu as pltpu
from jax.sharding import PartitionSpec as P

MESH = pl.DeviceIdType.MESH
F32 = jnp.float32
BF16 = jnp.bfloat16


def row_at(place, n):
    back = place // (n // 2)
    return 2 * place * (1 - back) + (2 * (n - 1 - place) + 1) * back


def kernel(n, tok_hbm, gate_hbm, up_hbm, down_hbm, out_ref, tok, weights, turned, rows_of, down, part, theirs, hid,
           total, other, send_y, from_y, load_sem, down_load, down_send, down_recv, tok_send, tok_recv,
           y_send, y_recv, part_send, part_recv, hid_send, hid_recv, sum_send, sum_recv, col_send, col_recv):
    row, col, core = lax.axis_index("row"), lax.axis_index("col"), lax.axis_index("depth")
    half = n // 2
    x, z = row % 2, row // 2
    place = z * (1 - x) + (n - 1 - z) * x
    ways = ({"row": row_at((place + 1) % n, n)}, {"row": row_at((place + n - 1) % n, n)})
    beside, partner = {"col": 1 - col}, {"depth": 1 - core}
    block = tok_hbm.shape[0]
    third = tok_hbm.shape[1] // 3
    units = gate_hbm.shape[0]
    share = units // 2

    def remote(src, dst, send, recv, to):
        return pltpu.make_async_remote_copy(src_ref=src, dst_ref=dst, send_sem=send, recv_sem=recv,
                                            device_id=to, device_id_type=MESH)

    loads = [pltpu.make_async_copy(tok_hbm.at[:, pl.ds(t * third, third)], tok.at[t, 0], load_sem.at[t])
             for t in range(3)]
    loads += [pltpu.make_async_copy(gate_hbm, weights.at[0], load_sem.at[3]),
              pltpu.make_async_copy(up_hbm, weights.at[1], load_sem.at[4]),
              pltpu.make_async_copy(down_hbm, turned, load_sem.at[5])]
    for copy in loads:
        copy.start()
    barrier = pltpu.get_barrier_semaphore()
    for peer in ways + (beside, partner):
        pl.semaphore_signal(barrier, inc=1, device_id=peer, device_id_type=MESH)
    pl.semaphore_wait(barrier, 4)
    for copy in loads[:3]:
        copy.wait()

    def slot(hop, way):
        return 0 if hop == 0 else 1 if hop == half else 2 * hop + way

    def rounds(hop, chunk):
        return (chunk,) if hop == half else (0, 1)

    started = []

    def go(copy):
        copy.start()
        started.append(copy)

    def tok_copy(hop, way, chunk):
        t = 2 * col if chunk == 0 else 1
        return remote(tok.at[t, slot(hop - 1, way)], tok.at[t, slot(hop, way)],
                      tok_send.at[way, hop - 1, chunk], tok_recv.at[way, hop - 1, chunk], ways[way])

    def y_copy(at, t):
        return remote(tok.at[t, at], tok.at[t, at], y_send.at[at], y_recv.at[at], beside)

    for chunk in (0, 1):
        for way in (0, 1):
            go(tok_copy(1, way, chunk))

    local_down, remote_down = [], []
    for i in range(half):
        keep = rows_of.at[pl.ds(i * units + core * share, share)]
        give = rows_of.at[pl.ds(i * units + (1 - core) * share, share)]
        dst = down.at[core * half + i]
        local_down.append(pltpu.make_async_copy(keep, dst, down_load.at[i]))
        remote_down.append(remote(give, dst, down_send.at[i], down_recv.at[i], partner))
    for copy in loads[3:]:
        copy.wait()

    @pl.loop(0, turned.shape[1] // 128)
    def _(step):
        at = pl.ds(pl.multiple_of(step * 128, 128), 128)
        rows_of[at, :] = turned[:, at].T

    for copy in local_down + remote_down:
        copy.start()

    def gate_up(group, slots, to):
        wide = block * len(slots)
        first = slots[0]

        @pl.loop(0, 4)
        def _(step):
            side, kind = step // 2, step % 2
            which = (1 - core) * (1 - side) + core * side
            rows = pl.ds(pl.multiple_of(which * share, 16), share)
            acc = None
            for t in range(3):
                seen = tok[t, first:first + len(slots)].reshape(wide, third)
                term = lax.dot_general(weights[kind, rows, t * third:(t + 1) * third], seen,
                                       (((1,), (1,)), ((), ())), preferred_element_type=F32)
                acc = term if acc is None else acc + term
            part[group, side, kind, :, :wide] = acc

        swap = remote(part.at[group, 0, :, :, pl.ds(0, wide)], theirs.at[group, :, :, pl.ds(0, wide)],
                      part_send.at[group], part_recv.at[group], partner)
        go(swap)
        swap.wait_recv()
        gate = part[group, 1, 0, :, :wide] + theirs[group, 0, :, :wide]
        up = part[group, 1, 1, :, :wide] + theirs[group, 1, :, :wide]
        hid[0, :, to:to + wide] = (gate / (1.0 + jnp.exp(-gate)) * up).astype(BF16)

    wide_piece = 2 * block

    def hid_copy(piece, hop, way):
        at = pl.ds((piece - 1) * wide_piece, wide_piece)
        return remote(hid.at[slot(hop - 1, way), :, at], hid.at[slot(hop, way), :, at],
                      hid_send.at[way, hop - 1, piece - 1], hid_recv.at[way, hop - 1, piece - 1], ways[way])

    def hid_rounds(piece, hop):
        return (piece % 2,) if hop == half else (0, 1)

    def add_down(at, source, piece):
        lanes = slice((piece - 1) * wide_piece, piece * wide_piece)
        term = lax.dot_general(hid[at, :, lanes], down[row_at(source, n)], (((0,), (0,)), ((), ())),
                               preferred_element_type=F32)
        before = source if piece == half else (source + n - piece) % n
        for k, token_block in enumerate((before, (source + piece) % n)):
            total[row_at(token_block, n)] += term[k * block:(k + 1) * block]

    def wave(number):
        for piece in range(1, half + 1):
            hop = number + 1 - piece
            if hop == 1:
                for way in (0, 1):
                    go(hid_copy(piece, 1, way))
            elif 2 <= hop <= half + 1:
                for way in hid_rounds(piece, hop - 1):
                    hid_copy(piece, hop - 1, way).wait_recv()
                    if hop <= half and way in hid_rounds(piece, hop):
                        go(hid_copy(piece, hop, way))
        for piece in range(1, half + 1):
            hop = number - piece
            if hop == 0:
                add_down(0, place, piece)
            elif hop == half:
                add_down(1, (place + half) % n, piece)
            elif 1 <= hop < half:
                @pl.loop(0, 2)
                def _(way):
                    add_down(2 * hop + way, (place + n - hop + 2 * hop * way) % n, piece)

    total[...] = jnp.zeros_like(total)
    for hop in range(1, half + 1):
        for chunk in (0, 1):
            for way in rounds(hop, chunk):
                tok_copy(hop, way, chunk).wait_recv()
                if hop < half and way in rounds(hop + 1, chunk):
                    go(tok_copy(hop + 1, way, chunk))
                if chunk == 0:
                    go(y_copy(slot(hop, way), 2 * col))
        if hop == 1:
            gate_up(0, [0], (half - 1) * wide_piece)
            for copy in local_down:
                copy.wait()
            for copy in remote_down:
                copy.wait()
        else:
            slots = [2 * (hop - 1), 2 * (hop - 1) + 1]
            for at in slots:
                y_copy(at, 2 - 2 * col).wait_recv()
            gate_up(hop - 1, slots, (hop - 2) * wide_piece)
            wave(hop - 1)
    y_copy(1, 2 - 2 * col).wait_recv()
    gate_up(half, [1], (half - 1) * wide_piece + block)
    for number in range(half, 2 * half + 1):
        wave(number)

    few = n // 4

    def sum_copy(side, k):
        c = 1 - col if side == 0 else col
        return remote(total.at[(c * 2 + 1 - core) * few + k], other.at[side, k],
                      sum_send.at[side, k], sum_recv.at[side, k], partner)

    def col_copy(k):
        return remote(send_y.at[k], from_y.at[k], col_send.at[k], col_recv.at[k], beside)

    for side in (0, 1):
        for k in range(few):
            go(sum_copy(side, k))
    for k in range(few):
        sum_copy(0, k).wait_recv()
        send_y[k] = (total[((1 - col) * 2 + core) * few + k] + other[0, k]).astype(BF16)
        go(col_copy(k))
    for k in range(few):
        sum_copy(1, k).wait_recv()
        mine = total[(col * 2 + core) * few + k] + other[1, k]
        col_copy(k).wait_recv()
        out_ref[k * block:(k + 1) * block] = (mine + from_y[k].astype(F32)).astype(BF16)
    for copy in started:
        copy.wait_send()


def partial_sums(n, tokens, gate_weight, up_weight, down_weight):
    block, width = tokens.shape
    units = gate_weight.shape[0]
    features = down_weight.shape[1]
    few = n // 4
    half, share = n // 2, units // 2
    every = n * block
    dma = pltpu.SemaphoreType.DMA
    return pl.pallas_call(
        functools.partial(kernel, n),
        out_shape=jax.ShapeDtypeStruct((every // 4, features), BF16),
        in_specs=[pl.BlockSpec(memory_space=pl.ANY)] * 4,
        out_specs=pl.BlockSpec(memory_space=pltpu.VMEM),
        scratch_shapes=[
            pltpu.VMEM((3, n, block, width // 3), BF16),
            pltpu.VMEM((2, units, width), BF16),
            pltpu.VMEM((features, down_weight.shape[0]), BF16),
            pltpu.VMEM((down_weight.shape[0], features), BF16),
            pltpu.VMEM((n, share, features), BF16),
            pltpu.VMEM((half + 1, 2, 2, share, 2 * block), F32),
            pltpu.VMEM((half + 1, 2, share, 2 * block), F32),
            pltpu.VMEM((n, share, every), BF16),
            pltpu.VMEM((n, block, features), F32),
            pltpu.VMEM((2, few, block, features), F32),
            pltpu.VMEM((few, block, features), BF16),
            pltpu.VMEM((few, block, features), BF16),
            dma((6,)),
            dma((half,)), dma((half,)), dma((half,)),
            dma((2, half, 2)), dma((2, half, 2)),
            dma((n,)), dma((n,)),
            dma((half + 1,)), dma((half + 1,)),
            dma((2, half, half)), dma((2, half, half)),
            dma((2, few)), dma((2, few)),
            dma((few,)), dma((few,)),
        ],
        compiler_params=pltpu.CompilerParams(
            collective_id=0, has_side_effects=True, vmem_limit_bytes=60 * 1024 * 1024
        ),
    )(tokens, gate_weight, up_weight, down_weight.T)


def send_out(mine, rows, cols, depths):
    quarters = cols * depths
    per = rows // quarters
    block = mine.shape[0] // per
    width = mine.shape[1]
    row = lax.axis_index("row")
    low = row % per
    got = jnp.zeros((block, per, width), jnp.bfloat16)
    for k in range(per):
        pairs = []
        for r in range(rows):
            for q in range(quarters):
                a, e = r // per, r % per
                to_row = q * per + (e + k) % per
                pairs.append((r * quarters + q, to_row * quarters + a))
        piece = lax.dynamic_slice_in_dim(mine, (low + k) % per * block, block, 0)
        piece = lax.ppermute(piece, ("row", "col", "depth"), pairs)
        got = lax.dynamic_update_slice_in_dim(got, piece[:, None], (low - k) % per, 1)
    return got.reshape(block, per * width)


def solution(mesh):
    rows, cols, depths = (mesh.shape[a] for a in ("row", "col", "depth"))

    def local(tokens, gate_weight, up_weight, down_weight):
        units = gate_weight.shape[0]
        every = lax.all_gather(tokens, "row", axis=0, tiled=True)
        down = down_weight.reshape(rows // depths, depths, units // depths, -1)
        down = lax.all_to_all(down, "depth", split_axis=1, concat_axis=0, tiled=True)
        down = down.reshape(rows, units // depths, -1)
        paired = jnp.stack([gate_weight, up_weight])
        sums = jnp.einsum("td,gfd->gtf", every, paired, preferred_element_type=jnp.float32)
        sums = lax.psum_scatter(sums, "depth", scatter_dimension=2, tiled=True)
        hidden = (jax.nn.silu(sums[0]) * sums[1]).astype(jnp.bfloat16)
        hidden = lax.all_gather(hidden, "row", axis=0)
        partial = jnp.einsum("rtk,rkc->tc", hidden, down, preferred_element_type=jnp.float32)
        mine = lax.psum_scatter(partial, ("col", "depth"), scatter_dimension=0, tiled=True)
        return send_out(mine.astype(BF16), rows, cols, depths)

    def fused(*args):
        return send_out(partial_sums(rows, *args), rows, cols, depths)

    in_specs = (
        P("row", "depth"),
        P(("col", "row"), "depth"),
        P(("col", "row"), "depth"),
        P(("col", "depth"), "row"),
    )
    out_specs = P("row", ("col", "depth"))
    small = cols == 2 and depths == 2 and rows % 4 == 0
    return jax.shard_map(fused if small else local, mesh=mesh, in_specs=in_specs, out_specs=out_specs, check_vma=False)
```

```python
import functools

import jax
import jax.numpy as jnp
from jax import lax
from jax.experimental import pallas as pl
from jax.experimental.pallas import tpu as pltpu
from jax.sharding import PartitionSpec as P

MESH = pl.DeviceIdType.MESH
F32 = jnp.float32
BF16 = jnp.bfloat16


def row_at(place, n):
    back = place // (n // 2)
    return 2 * place * (1 - back) + (2 * (n - 1 - place) + 1) * back


def kernel(n, tok_hbm, gate_hbm, up_hbm, down_hbm, out_ref, tok, weights, turned, rows_of, down, part, theirs, hid,
           total, other, send_y, from_y, load_sem, down_load, down_send, down_recv, tok_send, tok_recv,
           y_send, y_recv, part_send, part_recv, hid_send, hid_recv, sum_send, sum_recv, col_send, col_recv,
           done, land, passed, out_send, out_recv, pass_send, pass_recv):
    row, col, core = lax.axis_index("row"), lax.axis_index("col"), lax.axis_index("depth")
    half = n // 2
    x, z = row % 2, row // 2
    place = z * (1 - x) + (n - 1 - z) * x
    ways = ({"row": row_at((place + 1) % n, n)}, {"row": row_at((place + n - 1) % n, n)})
    beside, partner = {"col": 1 - col}, {"depth": 1 - core}
    block = tok_hbm.shape[0]
    third = tok_hbm.shape[1] // 3
    units = gate_hbm.shape[0]
    share = units // 2

    def remote(src, dst, send, recv, to):
        return pltpu.make_async_remote_copy(src_ref=src, dst_ref=dst, send_sem=send, recv_sem=recv,
                                            device_id=to, device_id_type=MESH)

    loads = [pltpu.make_async_copy(tok_hbm.at[:, pl.ds(t * third, third)], tok.at[t, 0], load_sem.at[t])
             for t in range(3)]
    loads += [pltpu.make_async_copy(gate_hbm, weights.at[0], load_sem.at[3]),
              pltpu.make_async_copy(up_hbm, weights.at[1], load_sem.at[4]),
              pltpu.make_async_copy(down_hbm, turned, load_sem.at[5])]
    for copy in loads:
        copy.start()
    barrier = pltpu.get_barrier_semaphore()
    for peer in ways + (beside, partner):
        pl.semaphore_signal(barrier, inc=1, device_id=peer, device_id_type=MESH)
    near = 1 - jnp.minimum((z // 2 - core) * (z // 2 - core) + (z % 2 - core) * (z % 2 - core), 1)
    sinks = [{"row": 4 * core + m, "depth": z % 2} for m in range(4)]
    feeds = [{"row": 4 * (m // 2) + 2 * core + m % 2, "depth": z // 2} for m in range(4)]
    away = [(row - peer["row"]) * (row - peer["row"]) + (core - peer["depth"]) * (core - peer["depth"])
            for peer in sinks + feeds]
    for peer, far in zip(sinks + feeds, away):
        @pl.when(far > 0)
        def _(peer=peer):
            pl.semaphore_signal(barrier, inc=1, device_id=peer, device_id_type=MESH)
    pl.semaphore_wait(barrier, 12 - 2 * near)
    for copy in loads[:3]:
        copy.wait()

    def slot(hop, way):
        return 0 if hop == 0 else 1 if hop == half else 2 * hop + way

    def rounds(hop, chunk):
        return (chunk,) if hop == half else (0, 1)

    started = []

    def go(copy):
        copy.start()
        started.append(copy)

    def tok_copy(hop, way, chunk):
        t = 2 * col if chunk == 0 else 1
        return remote(tok.at[t, slot(hop - 1, way)], tok.at[t, slot(hop, way)],
                      tok_send.at[way, hop - 1, chunk], tok_recv.at[way, hop - 1, chunk], ways[way])

    def y_copy(at, t):
        return remote(tok.at[t, at], tok.at[t, at], y_send.at[at], y_recv.at[at], beside)

    for chunk in (0, 1):
        for way in (0, 1):
            go(tok_copy(1, way, chunk))

    local_down, remote_down = [], []
    for i in range(half):
        keep = rows_of.at[pl.ds(i * units + core * share, share)]
        give = rows_of.at[pl.ds(i * units + (1 - core) * share, share)]
        dst = down.at[core * half + i]
        local_down.append(pltpu.make_async_copy(keep, dst, down_load.at[i]))
        remote_down.append(remote(give, dst, down_send.at[i], down_recv.at[i], partner))
    for copy in loads[3:]:
        copy.wait()

    @pl.loop(0, turned.shape[1] // 128)
    def _(step):
        at = pl.ds(pl.multiple_of(step * 128, 128), 128)
        rows_of[at, :] = turned[:, at].T

    for copy in local_down + remote_down:
        copy.start()

    def gate_up(group, slots, to):
        wide = block * len(slots)
        first = slots[0]

        @pl.loop(0, 4)
        def _(step):
            side, kind = step // 2, step % 2
            which = (1 - core) * (1 - side) + core * side
            rows = pl.ds(pl.multiple_of(which * share, 16), share)
            acc = None
            for t in range(3):
                seen = tok[t, first:first + len(slots)].reshape(wide, third)
                term = lax.dot_general(weights[kind, rows, t * third:(t + 1) * third], seen,
                                       (((1,), (1,)), ((), ())), preferred_element_type=F32)
                acc = term if acc is None else acc + term
            part[group, side, kind, :, :wide] = acc

        swap = remote(part.at[group, 0, :, :, pl.ds(0, wide)], theirs.at[group, :, :, pl.ds(0, wide)],
                      part_send.at[group], part_recv.at[group], partner)
        go(swap)
        swap.wait_recv()
        gate = part[group, 1, 0, :, :wide] + theirs[group, 0, :, :wide]
        up = part[group, 1, 1, :, :wide] + theirs[group, 1, :, :wide]
        hid[0, :, to:to + wide] = (gate / (1.0 + jnp.exp(-gate)) * up).astype(BF16)

    wide_piece = 2 * block

    def hid_copy(piece, hop, way):
        at = pl.ds((piece - 1) * wide_piece, wide_piece)
        return remote(hid.at[slot(hop - 1, way), :, at], hid.at[slot(hop, way), :, at],
                      hid_send.at[way, hop - 1, piece - 1], hid_recv.at[way, hop - 1, piece - 1], ways[way])

    def hid_rounds(piece, hop):
        return (piece % 2,) if hop == half else (0, 1)

    def add_down(at, source, piece):
        lanes = slice((piece - 1) * wide_piece, piece * wide_piece)
        term = lax.dot_general(hid[at, :, lanes], down[row_at(source, n)], (((0,), (0,)), ((), ())),
                               preferred_element_type=F32)
        before = source if piece == half else (source + n - piece) % n
        for k, token_block in enumerate((before, (source + piece) % n)):
            total[row_at(token_block, n)] += term[k * block:(k + 1) * block]

    def wave(number):
        for piece in range(1, half + 1):
            hop = number + 1 - piece
            if hop == 1:
                for way in (0, 1):
                    go(hid_copy(piece, 1, way))
            elif 2 <= hop <= half + 1:
                for way in hid_rounds(piece, hop - 1):
                    hid_copy(piece, hop - 1, way).wait_recv()
                    if hop <= half and way in hid_rounds(piece, hop):
                        go(hid_copy(piece, hop, way))
        for piece in range(1, half + 1):
            hop = number - piece
            if hop == 0:
                add_down(0, place, piece)
            elif hop == half:
                add_down(1, (place + half) % n, piece)
            elif 1 <= hop < half:
                @pl.loop(0, 2)
                def _(way):
                    add_down(2 * hop + way, (place + n - hop + 2 * hop * way) % n, piece)

    total[...] = jnp.zeros_like(total)
    for hop in range(1, half + 1):
        for chunk in (0, 1):
            for way in rounds(hop, chunk):
                tok_copy(hop, way, chunk).wait_recv()
                if hop < half and way in rounds(hop + 1, chunk):
                    go(tok_copy(hop + 1, way, chunk))
                if chunk == 0:
                    go(y_copy(slot(hop, way), 2 * col))
        if hop == 1:
            gate_up(0, [0], (half - 1) * wide_piece)
            for copy in local_down:
                copy.wait()
            for copy in remote_down:
                copy.wait()
        else:
            slots = [2 * (hop - 1), 2 * (hop - 1) + 1]
            for at in slots:
                y_copy(at, 2 - 2 * col).wait_recv()
            gate_up(hop - 1, slots, (hop - 2) * wide_piece)
            wave(hop - 1)
    y_copy(1, 2 - 2 * col).wait_recv()
    gate_up(half, [1], (half - 1) * wide_piece + block)
    for number in range(half, 2 * half + 1):
        wave(number)

    part_rows = block // 2

    def rows_in(c):
        return pl.ds(pl.multiple_of(c * part_rows, part_rows), part_rows)

    def sum_copy(side, m):
        c = 1 - col if side == 0 else col
        return remote(total.at[4 * (1 - core) + m, rows_in(c)], other.at[side, m],
                      sum_send.at[side, m], sum_recv.at[side, m], partner)

    def col_copy(m):
        return remote(send_y.at[m], from_y.at[m], col_send.at[m], col_recv.at[m], beside)

    spot = z // 2 * 2 + x

    def out_copy(m):
        return remote(done.at[m], land.at[spot], out_send.at[m], out_recv.at[spot], sinks[m])

    def landed(at):
        remote(done.at[0], land.at[at], out_send.at[0], out_recv.at[at], beside).wait_recv()

    def pass_copy(k):
        return remote(land.at[(1 - col) * 2 + k], passed.at[k], pass_send.at[k], pass_recv.at[k], beside)

    for side in (0, 1):
        for m in range(4):
            go(sum_copy(side, m))
    for m in range(4):
        sum_copy(0, m).wait_recv()
        send_y[m] = (total[4 * core + m, rows_in(1 - col)] + other[0, m]).astype(BF16)
        go(col_copy(m))
    for m in range(4):
        sum_copy(1, m).wait_recv()
        mine = total[4 * core + m, rows_in(col)] + other[1, m]
        col_copy(m).wait_recv()
        done[m] = (mine + from_y[m].astype(F32)).astype(BF16)

        @pl.when(away[m] > 0)
        def _():
            out_copy(m).start()

        @pl.when(away[m] == 0)
        def _():
            pltpu.make_async_copy(done.at[m], land.at[spot], out_recv.at[spot]).start()
    for k in (0, 1):
        landed((1 - col) * 2 + k)
        go(pass_copy(k))
    for k in (0, 1):
        landed(col * 2 + k)
        out_ref[k, rows_in(col)] = land[col * 2 + k]
    for k in (0, 1):
        pass_copy(k).wait_recv()
        out_ref[k, rows_in(1 - col)] = passed[k]
    for m in range(4):
        @pl.when(away[m] > 0)
        def _():
            out_copy(m).wait_send()
    for copy in started:
        copy.wait_send()


def partial_sums(n, tokens, gate_weight, up_weight, down_weight):
    block, width = tokens.shape
    units = gate_weight.shape[0]
    features = down_weight.shape[1]
    piece = block // 2
    half, share = n // 2, units // 2
    every = n * block
    dma = pltpu.SemaphoreType.DMA
    return pl.pallas_call(
        functools.partial(kernel, n),
        out_shape=jax.ShapeDtypeStruct((2, block, features), BF16),
        in_specs=[pl.BlockSpec(memory_space=pl.ANY)] * 4,
        out_specs=pl.BlockSpec(memory_space=pltpu.VMEM),
        scratch_shapes=[
            pltpu.VMEM((3, n, block, width // 3), BF16),
            pltpu.VMEM((2, units, width), BF16),
            pltpu.VMEM((features, down_weight.shape[0]), BF16),
            pltpu.VMEM((down_weight.shape[0], features), BF16),
            pltpu.VMEM((n, share, features), BF16),
            pltpu.VMEM((half + 1, 2, 2, share, 2 * block), F32),
            pltpu.VMEM((half + 1, 2, share, 2 * block), F32),
            pltpu.VMEM((n, share, every), BF16),
            pltpu.VMEM((n, block, features), F32),
            pltpu.VMEM((2, 4, piece, features), F32),
            pltpu.VMEM((4, piece, features), BF16),
            pltpu.VMEM((4, piece, features), BF16),
            dma((6,)),
            dma((half,)), dma((half,)), dma((half,)),
            dma((2, half, 2)), dma((2, half, 2)),
            dma((n,)), dma((n,)),
            dma((half + 1,)), dma((half + 1,)),
            dma((2, half, half)), dma((2, half, half)),
            dma((2, 4)), dma((2, 4)),
            dma((4,)), dma((4,)),
            pltpu.VMEM((4, piece, features), BF16),
            pltpu.VMEM((4, piece, features), BF16),
            pltpu.VMEM((2, piece, features), BF16),
            dma((4,)), dma((4,)), dma((2,)), dma((2,)),
        ],
        compiler_params=pltpu.CompilerParams(
            collective_id=0, has_side_effects=True, vmem_limit_bytes=60 * 1024 * 1024
        ),
    )(tokens, gate_weight, up_weight, down_weight.T)


def send_out(mine, rows, cols, depths):
    quarters = cols * depths
    per = rows // quarters
    block = mine.shape[0] // per
    width = mine.shape[1]
    row = lax.axis_index("row")
    low = row % per
    got = jnp.zeros((block, per, width), jnp.bfloat16)
    for k in range(per):
        pairs = []
        for r in range(rows):
            for q in range(quarters):
                a, e = r // per, r % per
                to_row = q * per + (e + k) % per
                pairs.append((r * quarters + q, to_row * quarters + a))
        piece = lax.dynamic_slice_in_dim(mine, (low + k) % per * block, block, 0)
        piece = lax.ppermute(piece, ("row", "col", "depth"), pairs)
        got = lax.dynamic_update_slice_in_dim(got, piece[:, None], (low - k) % per, 1)
    return got.reshape(block, per * width)


def solution(mesh):
    rows, cols, depths = (mesh.shape[a] for a in ("row", "col", "depth"))

    def local(tokens, gate_weight, up_weight, down_weight):
        units = gate_weight.shape[0]
        every = lax.all_gather(tokens, "row", axis=0, tiled=True)
        down = down_weight.reshape(rows // depths, depths, units // depths, -1)
        down = lax.all_to_all(down, "depth", split_axis=1, concat_axis=0, tiled=True)
        down = down.reshape(rows, units // depths, -1)
        paired = jnp.stack([gate_weight, up_weight])
        sums = jnp.einsum("td,gfd->gtf", every, paired, preferred_element_type=jnp.float32)
        sums = lax.psum_scatter(sums, "depth", scatter_dimension=2, tiled=True)
        hidden = (jax.nn.silu(sums[0]) * sums[1]).astype(jnp.bfloat16)
        hidden = lax.all_gather(hidden, "row", axis=0)
        partial = jnp.einsum("rtk,rkc->tc", hidden, down, preferred_element_type=jnp.float32)
        mine = lax.psum_scatter(partial, ("col", "depth"), scatter_dimension=0, tiled=True)
        return send_out(mine.astype(BF16), rows, cols, depths)

    def fused(*args):
        return jnp.concatenate(list(partial_sums(rows, *args)), axis=1)

    in_specs = (
        P("row", "depth"),
        P(("col", "row"), "depth"),
        P(("col", "row"), "depth"),
        P(("col", "depth"), "row"),
    )
    out_specs = P("row", ("col", "depth"))
    small = cols == 2 and depths == 2 and rows == 8
    return jax.shard_map(fused if small else local, mesh=mesh, in_specs=in_specs, out_specs=out_specs, check_vma=False)
```
